32 devices in a mesh: grp: 4 (over y, x), mem: 8 (over z, core).
Axes of the slice: x: 2, y: 2, z: 4, core: 2. Of those that a mesh axis runs over, the one named last changes fastest.
Arguments:
- values: bfloat16 [32, 8, 32, 128], P(('grp', 'mem')), may hold values from -6 to 6
- slots: int32 [32, 8, 32], P(('grp', 'mem')), may hold values from 0 to 7167
- counts: int32 [32, 8], P(('grp', 'mem')), may hold values from 0 to 32, as said below
Outputs:
- averaged: float32 [57344, 128], P('mem')
- returned: bfloat16 [32, 8, 32, 128], P(('grp', 'mem'))
The draws below stay inside these ranges and needn't reach their ends.
Inputs may be any that keep to these rules, and one draw needn't show every extreme that they name: `counts`: every device has at least one list with exactly 32 valid entries.
All inputs are finite; a program needn't handle non-finite values.
Results may differ from the reference program's by a relative error of at most 0.0024.
Values may be sent and summed in bfloat16 or wider, within the bound.
A program may use at most 64 MiB of HBM per device.

```python
import jax
import jax.numpy as jnp

BLOCK = 128
BUCKET = 7168
CAP = 32
SENDERS = 32
N_MEM = 8


def draw_counts(key, part):
    key_load, key_base, key_full = jax.random.split(jax.random.fold_in(key, 7), 3)
    owner_load = jax.random.randint(key_load, (1, N_MEM), 1, 5)
    base_count = jax.random.randint(key_base, (SENDERS, N_MEM), 0, CAP + 1)
    scaled = jnp.minimum(base_count * owner_load // 2, CAP)
    full_list = jax.random.randint(key_full, (SENDERS, 1), 0, N_MEM)
    columns = jnp.arange(N_MEM, dtype=jnp.int32)[None, :]
    return jnp.where(columns == full_list, CAP, scaled).astype(jnp.int32)


def touch_ends(result, own_key, smallest, top_value):
    longest = result.shape.index(max(result.shape))
    spots = []
    for shift in (0, 1):
        where = [jax.random.randint(jax.random.fold_in(own_key, axis), (), 0, length) for axis, length in enumerate(result.shape)]
        where[longest] = (where[longest] + shift) % result.shape[longest]
        spots.append(tuple(where))
    return result.at[spots[0]].set(smallest).at[spots[1]].set(top_value)


def level_of(own_key, dims, cuts, low, high):
    def one(dim, parts):
        draws = jax.random.uniform(jax.random.fold_in(jax.random.fold_in(own_key, 6), dim), (parts,), jnp.float32, low / len(cuts), high / len(cuts))
        return jnp.repeat(jnp.exp(draws), dims[dim] // parts).reshape((-1,) + (1,) * (len(dims) - dim - 1))

    factor_of = one(*cuts[0])
    for cut in cuts[1:]:
        factor_of = factor_of * one(*cut)
    return factor_of


def noise(own_key, shape, deviation, limit, cuts=(), kind=jnp.bfloat16):
    drawn = deviation * jax.random.normal(own_key, shape, jnp.float32)
    if cuts:
        drawn = drawn * level_of(own_key, shape, cuts, -0.22, 0.18)
    return jnp.clip(drawn, -limit, limit).astype(kind)


def setup_inputs(seed: int = 0) -> dict:
    key_list = jax.random.split(jax.random.key(seed), 4)
    return {
        "values": noise(key_list[0], (SENDERS, N_MEM, CAP, BLOCK), 1.0, 6.0, ((0, 32),)),
        "slots": touch_ends(jax.random.randint(key_list[1], (SENDERS, N_MEM, CAP), 0, BUCKET), jax.random.fold_in(key_list[1], 1), 0, BUCKET - 1).astype(jnp.int32),
        "counts": draw_counts(jax.random.fold_in(key_list[3], 71), 0),
    }


def reference(values, slots, counts):
    is_valid = jnp.arange(CAP, dtype=jnp.int32)[None, None, :] < counts[:, :, None]
    target = (jnp.arange(N_MEM, dtype=jnp.int32)[None, :, None] * BUCKET + slots).reshape(-1)
    masked = jnp.where(is_valid[..., None], values.astype(jnp.float32), jnp.float32(0.0)).reshape(-1, BLOCK)
    slot_sums = jax.ops.segment_sum(masked, target, num_segments=N_MEM * BUCKET)
    slot_count = jax.ops.segment_sum(is_valid.reshape(-1).astype(jnp.float32), target, num_segments=N_MEM * BUCKET)
    averaged = slot_sums / jnp.maximum(slot_count, jnp.float32(1.0))[:, None]
    picked = jnp.take(averaged, target, axis=0).reshape(values.shape)
    returned = jnp.where(is_valid[..., None], picked, jnp.float32(0.0)).astype(jnp.bfloat16)
    return averaged, returned
```

```python
import functools

import jax
import jax.numpy as jnp
from jax import lax
from jax.experimental import pallas as pl
from jax.experimental.pallas import tpu as pltpu
from jax.sharding import PartitionSpec as P

BUCKET = 7168
LANES = 128
ROWS = 256
WIDE = 1024


def exchange_kernel(
    groups, members, cap,
    values_ref, slots_ref, counts_ref,
    avg_ref, lane_ref, back_ref,
    got, got_slots, own_slots, lane_f, ret,
    v_send, v_recv, s_send, s_recv,
    fv_send, fv_recv, fs_send, fs_recv,
    r_send, r_recv, local_sem,
):
    g = lax.axis_index("grp")
    m = lax.axis_index("mem")
    total = groups * members * cap
    per_row = LANES // cap

    barrier = pltpu.get_barrier_semaphore()
    for step in range(1, members):
        pl.semaphore_signal(barrier, inc=1, device_id={"mem": lax.rem(m + step, members)})
    for step in range(1, groups):
        pl.semaphore_signal(barrier, inc=1, device_id={"grp": lax.rem(g + step, groups)})

    raw = slots_ref[0]
    shown = jnp.concatenate([raw] * per_row, axis=1)
    row_id = lax.broadcasted_iota(jnp.int32, (members, LANES), 0)
    entry = lax.rem(lax.broadcasted_iota(jnp.int32, (members, LANES), 1), cap)
    limit = jnp.zeros((members, LANES), jnp.int32)
    for k in range(members):
        limit = jnp.where(row_id == k, counts_ref[0, k], limit)
    masked = jnp.where(entry < limit, shown, -1)
    for k in range(members):
        own_slots[k] = masked[k : k + 1, :]

    pl.semaphore_wait(barrier, members - 1 + groups - 1)

    mine = g * members + m

    def to_member(step):
        peer = lax.rem(m + step, members)
        return (
            pltpu.make_async_remote_copy(
                values_ref.at[0, peer], got.at[mine], v_send.at[step], v_recv.at[step],
                device_id={"mem": peer},
            ),
            pltpu.make_async_remote_copy(
                own_slots.at[peer], got_slots.at[mine], s_send.at[step], s_recv.at[step],
                device_id={"mem": peer},
            ),
        )

    def from_member(step):
        src = lax.rem(m + members - step, members)
        at = g * members + src
        return (
            pltpu.make_async_remote_copy(
                values_ref.at[0, src], got.at[at], v_send.at[step], v_recv.at[step],
                device_id={"mem": src},
            ),
            pltpu.make_async_remote_copy(
                own_slots.at[src], got_slots.at[at], s_send.at[step], s_recv.at[step],
                device_id={"mem": src},
            ),
        )

    def to_group(step, hop):
        src = lax.rem(m + members - step, members)
        at = g * members + src
        peer = lax.rem(g + hop, groups)
        return (
            pltpu.make_async_remote_copy(
                got.at[at], got.at[at], fv_send.at[step, hop], fv_recv.at[step, hop],
                device_id={"grp": peer},
            ),
            pltpu.make_async_remote_copy(
                got_slots.at[at], got_slots.at[at], fs_send.at[step, hop], fs_recv.at[step, hop],
                device_id={"grp": peer},
            ),
        )

    def from_group(step, hop):
        src = lax.rem(m + members - step, members)
        peer = lax.rem(g + groups - hop, groups)
        at = peer * members + src
        return (
            pltpu.make_async_remote_copy(
                got.at[at], got.at[at], fv_send.at[step, hop], fv_recv.at[step, hop],
                device_id={"grp": peer},
            ),
            pltpu.make_async_remote_copy(
                got_slots.at[at], got_slots.at[at], fs_send.at[step, hop], fs_recv.at[step, hop],
                device_id={"grp": peer},
            ),
        )

    local_v = pltpu.make_async_copy(values_ref.at[0, m], got.at[mine], local_sem.at[0])
    local_s = pltpu.make_async_copy(own_slots.at[m], got_slots.at[mine], local_sem.at[1])
    local_v.start()
    local_s.start()

    def each(low, high, body):
        if high - low <= 8:
            for k in range(low, high):
                body(k)
        else:
            lax.fori_loop(low, high, lambda k, c: (body(k), c)[1], 0)

    def start_members(step):
        for copy in to_member(step):
            copy.start()

    each(1, members, start_members)

    local_v.wait()
    local_s.wait()

    def forward(step):
        for hop in range(1, groups):
            for copy in to_group(step, hop):
                copy.start()

    forward(0)

    def pass_on(step):
        for copy in from_member(step):
            copy.wait_recv()
        forward(step)

    each(1, members, pass_on)

    def land(step):
        for hop in range(1, groups):
            for copy in from_group(step, hop):
                copy.wait_recv()

    each(0, members, land)

    lane = lax.broadcasted_iota(jnp.int32, (1, LANES), 1)

    def pack(k):
        row = got_slots[k * per_row]
        for q in range(1, per_row):
            row = jnp.where(lane >= q * cap, got_slots[k * per_row + q], row)
        lane_ref[pl.ds(k, 1), :] = row
        lane_f[pl.ds(k, 1), :] = row.astype(jnp.float32)

    each(0, total // LANES, pack)

    wide = min(WIDE, total)
    senders_wide = wide // cap
    halves = ROWS // LANES

    def block(b):
        columns = []
        for h in range(halves):
            row = lane_f[pl.ds(b * halves + h, 1), :]
            row = jnp.where(row < 0, -2.0, row)
            columns.append(jnp.transpose(jnp.broadcast_to(row, (LANES, LANES))))
        column = jnp.concatenate(columns, axis=0)

        def part(w):
            same = []
            for l in range(wide // LANES):
                row = lane_f[pl.ds(w * (wide // LANES) + l, 1), :]
                same.append(jnp.where(column == row, 1.0, 0.0).astype(jnp.bfloat16))
            onehot = jnp.concatenate(same, axis=1)
            rows = got[pl.ds(w * senders_wide, senders_wide)].reshape(wide, LANES)
            rows = jnp.concatenate([rows, jnp.ones((wide, LANES), jnp.bfloat16)], axis=1)
            return jnp.dot(onehot, rows, preferred_element_type=jnp.float32)

        if total == wide:
            acc = part(0)
        else:
            acc = lax.fori_loop(
                0, total // wide, lambda w, a: a + part(w), jnp.zeros((ROWS, 2 * LANES), jnp.float32)
            )
        avg = acc[:, :LANES] / jnp.maximum(acc[:, LANES:], 1.0)
        avg_ref[pl.ds(b * ROWS, ROWS), :] = avg
        return avg

    blocks_each = members * cap // ROWS
    senders_each = ROWS // cap

    def own_block(t):
        avg = block(g * blocks_each + t)
        ret[pl.ds(t * senders_each, senders_each)] = avg.astype(jnp.bfloat16).reshape(
            senders_each, cap, LANES
        )

    each(0, blocks_each, own_block)

    def back_to(step):
        peer = lax.rem(m + step, members)
        return pltpu.make_async_remote_copy(
            ret.at[peer], back_ref.at[m], r_send.at[step], r_recv.at[step],
            device_id={"mem": peer},
        )

    def back_from(step):
        src = lax.rem(m + members - step, members)
        return pltpu.make_async_remote_copy(
            ret.at[src], back_ref.at[src], r_send.at[step], r_recv.at[step],
            device_id={"mem": src},
        )

    each(1, members, lambda step: back_to(step).start())
    local_r = pltpu.make_async_copy(ret.at[m], back_ref.at[m], local_sem.at[2])
    local_r.start()

    for q in range(1, groups):
        other = lax.rem(g + q, groups)
        each(0, blocks_each, lambda t, other=other: (block(other * blocks_each + t), None)[1])

    def finish(step):
        for copy in to_member(step):
            copy.wait_send()
        back_to(step).wait_send()
        back_from(step).wait_recv()

    def finish_forward(step):
        for hop in range(1, groups):
            for copy in to_group(step, hop):
                copy.wait_send()

    each(0, members, finish_forward)
    local_r.wait()
    each(1, members, finish)


def place_kernel(total, avg_ref, slot_ref, back_ref, out_ref, returned_ref, table, sems):
    unroll = 16
    table[...] = jnp.zeros_like(table)
    returned_ref[...] = back_ref[...]

    def step(i, carry):
        base = pl.multiple_of(i * unroll, unroll)
        row = base // LANES
        col = lax.rem(base, LANES)
        for k in range(unroll):
            s = slot_ref[row, col + k]
            s = jnp.where(s < 0, BUCKET, s)
            table[pl.ds(s, 1), :] = avg_ref[pl.ds(base + k, 1), :]
        return carry

    lax.fori_loop(0, total // unroll, step, 0)
    pieces = sems.shape[0]
    size = BUCKET // pieces
    copies = [
        pltpu.make_async_copy(
            table.at[pl.ds(k * size, size)], out_ref.at[pl.ds(k * size, size)], sems.at[k]
        )
        for k in range(pieces)
    ]
    for copy in copies:
        copy.start()
    for copy in copies:
        copy.wait()


def per_device(groups, members, values, slots, counts):
    cap, lanes = values.shape[2:]
    total = groups * members * cap
    vmem = pl.BlockSpec(memory_space=pltpu.VMEM)
    smem = pl.BlockSpec(memory_space=pltpu.SMEM)
    dma = pltpu.SemaphoreType.DMA
    avg, lane_slots, back = pl.pallas_call(
        functools.partial(exchange_kernel, groups, members, cap),
        out_shape=(
            jax.ShapeDtypeStruct((total, lanes), jnp.float32),
            jax.ShapeDtypeStruct((total // LANES, LANES), jnp.int32),
            jax.ShapeDtypeStruct((members, cap, lanes), jnp.bfloat16),
        ),
        in_specs=[vmem, vmem, smem],
        out_specs=(vmem, vmem, vmem),
        scratch_shapes=[
            pltpu.VMEM((groups * members, cap, lanes), jnp.bfloat16),
            pltpu.VMEM((groups * members, 1, LANES), jnp.int32),
            pltpu.VMEM((members, 1, LANES), jnp.int32),
            pltpu.VMEM((total // LANES, LANES), jnp.float32),
            pltpu.VMEM((members, cap, lanes), jnp.bfloat16),
            dma((members,)), dma((members,)), dma((members,)), dma((members,)),
            dma((members, groups)), dma((members, groups)),
            dma((members, groups)), dma((members, groups)),
            dma((members,)), dma((members,)), dma((3,)),
        ],
        compiler_params=pltpu.CompilerParams(collective_id=0, has_side_effects=True),
    )(values, slots, counts)
    averaged, returned = pl.pallas_call(
        functools.partial(place_kernel, total),
        out_shape=(
            jax.ShapeDtypeStruct((BUCKET, lanes), jnp.float32),
            jax.ShapeDtypeStruct((members, cap, lanes), jnp.bfloat16),
        ),
        in_specs=[vmem, smem, vmem],
        out_specs=(pl.BlockSpec(memory_space=pl.ANY), vmem),
        scratch_shapes=[pltpu.VMEM((BUCKET + 8, lanes), jnp.float32), dma((4,))],
    )(avg, lane_slots, back)
    return averaged, returned[None]


def solution(mesh):
    return jax.shard_map(
        functools.partial(per_device, mesh.shape["grp"], mesh.shape["mem"]),
        mesh=mesh,
        in_specs=(
            P(("grp", "mem"), None, None, None),
            P(("grp", "mem"), None, None),
            P(("grp", "mem"), None),
        ),
        out_specs=(P("mem", None), P(("grp", "mem"), None, None, None)),
        check_vma=False,
    )
```

```python
import functools

import jax
import jax.numpy as jnp
from jax import lax
from jax.experimental import pallas as pl
from jax.experimental.pallas import tpu as pltpu
from jax.sharding import PartitionSpec as P

BUCKET = 7168
LANES = 128
ROWS = 256
WIDE = 1024
EXTRA = 8


def exchange_kernel(
    groups, members, cap,
    values_ref, slots_ref, counts_ref,
    avg_ref, lane_ref, back_ref,
    got, pay, slots_v, counts_s, lane_i, lane_f, avg_v, ret,
    v_send, v_recv, f_send, f_recv, r_send, r_recv, local_sem, avg_sem,
):
    g = lax.axis_index("grp")
    m = lax.axis_index("mem")
    total = groups * members * cap
    per_row = LANES // cap

    def each(low, high, body):
        if high - low <= 8:
            for k in range(low, high):
                body(k)
        else:
            lax.fori_loop(low, high, lambda k, c: (body(k), c)[1], 0)

    barrier = pltpu.get_barrier_semaphore()
    for step in range(1, members):
        pl.semaphore_signal(barrier, inc=1, device_id={"mem": lax.rem(m + step, members)})
    for step in range(1, groups):
        pl.semaphore_signal(barrier, inc=1, device_id={"grp": lax.rem(g + step, groups)})

    load_v = pltpu.make_async_copy(values_ref.at[0], pay.at[:, pl.ds(0, cap), :], local_sem.at[0])
    load_s = pltpu.make_async_copy(slots_ref.at[0], slots_v, local_sem.at[1])
    load_c = pltpu.make_async_copy(counts_ref, counts_s, local_sem.at[2])
    load_c.start()
    load_s.start()
    load_v.start()
    load_c.wait()
    load_s.wait()

    raw = slots_v[...]
    shown = jnp.concatenate([raw] * per_row, axis=1)
    row_id = lax.broadcasted_iota(jnp.int32, (members, LANES), 0)
    entry = lax.rem(lax.broadcasted_iota(jnp.int32, (members, LANES), 1), cap)
    limit = jnp.zeros((members, LANES), jnp.int32)
    for k in range(members):
        limit = jnp.where(row_id == k, counts_s[0, k], limit)
    masked = jnp.where(entry < limit, shown, -LANES)
    high = (masked >> 7).astype(jnp.float32)
    low = (masked & (LANES - 1)).astype(jnp.float32)
    part_id = lax.broadcasted_iota(jnp.int32, (EXTRA, LANES), 0)
    for k in range(members):
        both = jnp.where(part_id == 0, high[k : k + 1, :], low[k : k + 1, :])
        pay[k, cap:, :] = both.astype(jnp.bfloat16)
    load_v.wait()

    pl.semaphore_wait(barrier, members - 1 + groups - 1)

    mine = g * members + m

    def to_member(step):
        peer = lax.rem(m + step, members)
        return pltpu.make_async_remote_copy(
            pay.at[peer], got.at[mine], v_send.at[step], v_recv.at[step],
            device_id={"mem": peer},
        )

    def from_member(step):
        src = lax.rem(m + members - step, members)
        return pltpu.make_async_remote_copy(
            pay.at[src], got.at[g * members + src], v_send.at[step], v_recv.at[step],
            device_id={"mem": src},
        )

    def to_group(step, hop):
        src = lax.rem(m + members - step, members)
        at = g * members + src
        return pltpu.make_async_remote_copy(
            got.at[at], got.at[at], f_send.at[step, hop], f_recv.at[step, hop],
            device_id={"grp": lax.rem(g + hop, groups)},
        )

    def from_group(step, hop):
        src = lax.rem(m + members - step, members)
        peer = lax.rem(g + groups - hop, groups)
        at = peer * members + src
        return pltpu.make_async_remote_copy(
            got.at[at], got.at[at], f_send.at[step, hop], f_recv.at[step, hop],
            device_id={"grp": peer},
        )

    local_v = pltpu.make_async_copy(pay.at[m], got.at[mine], local_sem.at[0])
    local_v.start()
    each(1, members, lambda step: to_member(step).start())
    local_v.wait()

    def forward(step):
        for hop in range(1, groups):
            to_group(step, hop).start()

    forward(0)

    def pass_on(step):
        from_member(step).wait_recv()
        forward(step)

    each(1, members, pass_on)

    def land(step):
        for hop in range(1, groups):
            from_group(step, hop).wait_recv()

    each(0, members, land)

    lane = lax.broadcasted_iota(jnp.int32, (1, LANES), 1)

    def slots_of(sender):
        halves = got[sender, pl.ds(cap, EXTRA), :].astype(jnp.float32)
        return halves[0:1, :] * float(LANES) + halves[1:2, :]

    def pack(k):
        row = slots_of(k * per_row)
        for q in range(1, per_row):
            row = jnp.where(lane >= q * cap, slots_of(k * per_row + q), row)
        lane_i[pl.ds(k, 1), :] = jnp.where(row < 0, float(BUCKET), row).astype(jnp.int32)
        lane_f[pl.ds(k, 1), :] = row

    each(0, total // LANES, pack)
    store_lane = pltpu.make_async_copy(lane_i, lane_ref, local_sem.at[1])
    store_lane.start()

    wide = min(WIDE, total)
    senders_wide = wide // cap
    halves = ROWS // LANES

    def block(b):
        columns = []
        for h in range(halves):
            row = lane_f[pl.ds(b * halves + h, 1), :]
            row = jnp.where(row < 0, -2.0, row)
            columns.append(jnp.transpose(jnp.broadcast_to(row, (LANES, LANES))))
        column = jnp.concatenate(columns, axis=0)

        def part(w):
            same = []
            for l in range(wide // LANES):
                row = lane_f[pl.ds(w * (wide // LANES) + l, 1), :]
                same.append(jnp.where(column == row, 1.0, 0.0).astype(jnp.bfloat16))
            onehot = jnp.concatenate(same, axis=1)
            rows = got[pl.ds(w * senders_wide, senders_wide), :cap, :].reshape(wide, LANES)
            rows = jnp.concatenate([rows, jnp.ones((wide, LANES), jnp.bfloat16)], axis=1)
            return jnp.dot(onehot, rows, preferred_element_type=jnp.float32)

        if total == wide:
            acc = part(0)
        else:
            acc = lax.fori_loop(
                0, total // wide, lambda w, a: a + part(w), jnp.zeros((ROWS, 2 * LANES), jnp.float32)
            )
        avg = acc[:, :LANES] / jnp.maximum(acc[:, LANES:], 1.0)
        avg_v[pl.ds(b * ROWS, ROWS), :] = avg
        return avg

    def store_avg(q):
        at = pl.ds(lax.rem(g + q, groups) * members * cap, members * cap)
        return pltpu.make_async_copy(avg_v.at[at], avg_ref.at[at], avg_sem.at[q])

    blocks_each = members * cap // ROWS
    senders_each = ROWS // cap

    def own_block(t):
        avg = block(g * blocks_each + t)
        ret[pl.ds(t * senders_each, senders_each)] = avg.astype(jnp.bfloat16).reshape(
            senders_each, cap, LANES
        )

    each(0, blocks_each, own_block)

    def back_to(step):
        peer = lax.rem(m + step, members)
        return pltpu.make_async_remote_copy(
            ret.at[peer], back_ref.at[m], r_send.at[step], r_recv.at[step],
            device_id={"mem": peer},
        )

    def back_from(step):
        src = lax.rem(m + members - step, members)
        return pltpu.make_async_remote_copy(
            ret.at[src], back_ref.at[src], r_send.at[step], r_recv.at[step],
            device_id={"mem": src},
        )

    each(1, members, lambda step: back_to(step).start())
    local_r = pltpu.make_async_copy(ret.at[m], back_ref.at[m], local_sem.at[2])
    local_r.start()
    store_avg(0).start()

    for q in range(1, groups):
        other = lax.rem(g + q, groups)
        each(0, blocks_each, lambda t, other=other: (block(other * blocks_each + t), None)[1])
        store_avg(q).start()

    def finish_forward(step):
        for hop in range(1, groups):
            to_group(step, hop).wait_send()

    each(0, members, finish_forward)
    each(1, members, lambda step: to_member(step).wait_send())
    store_lane.wait()
    for q in range(groups):
        store_avg(q).wait()
    local_r.wait()
    each(1, members, lambda step: back_to(step).wait_send())
    each(1, members, lambda step: back_from(step).wait_recv())


def place_kernel(total, avg_ref, slot_ref, back_ref, out_ref, returned_ref, table, rows, slot_s, back_v, in_sem, sems):
    unroll = 32
    load_s = pltpu.make_async_copy(slot_ref, slot_s, in_sem.at[0])
    load_a = pltpu.make_async_copy(avg_ref, rows, in_sem.at[1])
    load_b = pltpu.make_async_copy(back_ref, back_v, in_sem.at[2])
    store_b = pltpu.make_async_copy(back_v, returned_ref, in_sem.at[3])
    load_s.start()
    load_a.start()
    load_b.start()
    table[...] = jnp.zeros_like(table)
    load_s.wait()
    load_a.wait()
    load_b.wait()
    store_b.start()

    def step(i, carry):
        base = pl.multiple_of(i * unroll, unroll)
        row = base // LANES
        col = lax.rem(base, LANES)
        for k in range(unroll):
            s = slot_s[row, col + k]
            table[pl.ds(s, 1), :] = rows[pl.ds(base + k, 1), :]
        return carry

    lax.fori_loop(0, total // unroll, step, 0)
    pieces = sems.shape[0]
    size = BUCKET // pieces
    copies = [
        pltpu.make_async_copy(
            table.at[pl.ds(k * size, size)], out_ref.at[pl.ds(k * size, size)], sems.at[k]
        )
        for k in range(pieces)
    ]
    for copy in copies:
        copy.start()
    store_b.wait()
    for copy in copies:
        copy.wait()


def per_device(groups, members, values, slots, counts):
    cap, lanes = values.shape[2:]
    total = groups * members * cap
    hbm = pl.BlockSpec(memory_space=pl.ANY)
    dma = pltpu.SemaphoreType.DMA
    avg, lane_slots, back = pl.pallas_call(
        functools.partial(exchange_kernel, groups, members, cap),
        out_shape=(
            jax.ShapeDtypeStruct((total, lanes), jnp.float32),
            jax.ShapeDtypeStruct((total // LANES, LANES), jnp.int32),
            jax.ShapeDtypeStruct((members, cap, lanes), jnp.bfloat16),
        ),
        in_specs=[hbm, hbm, hbm],
        out_specs=(hbm, hbm, hbm),
        scratch_shapes=[
            pltpu.VMEM((groups * members, cap + EXTRA, lanes), jnp.bfloat16),
            pltpu.VMEM((members, cap + EXTRA, lanes), jnp.bfloat16),
            pltpu.VMEM((members, cap), jnp.int32),
            pltpu.SMEM((1, members), jnp.int32),
            pltpu.VMEM((total // LANES, LANES), jnp.int32),
            pltpu.VMEM((total // LANES, LANES), jnp.float32),
            pltpu.VMEM((total, lanes), jnp.float32),
            pltpu.VMEM((members, cap, lanes), jnp.bfloat16),
            dma((members,)), dma((members,)),
            dma((members, groups)), dma((members, groups)),
            dma((members,)), dma((members,)), dma((3,)), dma((groups,)),
        ],
        compiler_params=pltpu.CompilerParams(collective_id=0, has_side_effects=True),
    )(values, slots, counts)
    averaged, returned = pl.pallas_call(
        functools.partial(place_kernel, total),
        out_shape=(
            jax.ShapeDtypeStruct((BUCKET, lanes), jnp.float32),
            jax.ShapeDtypeStruct((members, cap, lanes), jnp.bfloat16),
        ),
        in_specs=[hbm, hbm, hbm],
        out_specs=(hbm, hbm),
        scratch_shapes=[
            pltpu.VMEM((BUCKET + 8, lanes), jnp.float32),
            pltpu.VMEM((total, lanes), jnp.float32),
            pltpu.SMEM((total // LANES, LANES), jnp.int32),
            pltpu.VMEM((members, cap, lanes), jnp.bfloat16),
            dma((4,)), dma((8,)),
        ],
    )(avg, lane_slots, back)
    return averaged, returned[None]


def solution(mesh):
    return jax.shard_map(
        functools.partial(per_device, mesh.shape["grp"], mesh.shape["mem"]),
        mesh=mesh,
        in_specs=(
            P(("grp", "mem"), None, None, None),
            P(("grp", "mem"), None, None),
            P(("grp", "mem"), None),
        ),
        out_specs=(P("mem", None), P(("grp", "mem"), None, None, None)),
        check_vma=False,
    )
```

```python
import functools

import jax
import jax.numpy as jnp
from jax import lax
from jax.experimental import pallas as pl
from jax.experimental.pallas import tpu as pltpu
from jax.sharding import PartitionSpec as P

BUCKET = 7168
LANES = 128
ROWS = 256
WIDE = 1024


def partner(index, step, count):
    if count & (count - 1):
        return None
    bit = 1
    while bit < count:
        flip = (step // bit) % 2
        index = index + flip * bit * (1 - 2 * ((index // bit) % 2))
        bit *= 2
    return index


def target(index, step, count):
    paired = partner(index, step, count)
    return lax.rem(index + step, count) if paired is None else paired


def origin(index, step, count):
    paired = partner(index, step, count)
    return lax.rem(index + count - step, count) if paired is None else paired


def exchange_kernel(
    groups, members, cap,
    values_ref, slots_ref, counts_ref,
    avg_ref, lane_ref, back_ref,
    got, got_slots, vals, own_slots, slots_v, counts_s, lane_i, lane_f, same_v, avg_v, ret,
    v_send, v_recv, s_send, s_recv, f_send, f_recv, fs_send, fs_recv,
    r_send, r_recv, local_sem, avg_sem,
):
    g = lax.axis_index("grp")
    m = lax.axis_index("mem")
    total = groups * members * cap
    per_row = LANES // cap

    def each(low, high, body):
        if high - low <= 8:
            for k in range(low, high):
                body(k)
        else:
            lax.fori_loop(low, high, lambda k, c: (body(k), c)[1], 0)

    barrier = pltpu.get_barrier_semaphore()
    for step in range(1, members):
        pl.semaphore_signal(barrier, inc=1, device_id={"mem": lax.rem(m + step, members)})
    for step in range(1, groups):
        pl.semaphore_signal(barrier, inc=1, device_id={"grp": lax.rem(g + step, groups)})

    load_v = pltpu.make_async_copy(values_ref.at[0], vals, local_sem.at[0])
    load_s = pltpu.make_async_copy(slots_ref.at[0], slots_v, local_sem.at[1])
    load_c = pltpu.make_async_copy(counts_ref, counts_s, local_sem.at[2])
    load_c.start()
    load_s.start()
    load_v.start()
    load_c.wait()
    load_s.wait()

    raw = slots_v[...]
    shown = jnp.concatenate([raw] * per_row, axis=1)
    row_id = lax.broadcasted_iota(jnp.int32, (members, LANES), 0)
    entry = lax.rem(lax.broadcasted_iota(jnp.int32, (members, LANES), 1), cap)
    limit = jnp.zeros((members, LANES), jnp.int32)
    for k in range(members):
        limit = jnp.where(row_id == k, counts_s[0, k], limit)
    masked = jnp.where(entry < limit, shown, -1)
    for k in range(members):
        own_slots[k] = masked[k : k + 1, :]
    load_v.wait()

    pl.semaphore_wait(barrier, members - 1 + groups - 1)

    mine = g * members + m

    def slots_to(step):
        peer = target(m, step, members)
        return pltpu.make_async_remote_copy(
            own_slots.at[peer], got_slots.at[mine], s_send.at[step], s_recv.at[step],
            device_id={"mem": peer},
        )

    def slots_from(step):
        src = origin(m, step, members)
        return pltpu.make_async_remote_copy(
            own_slots.at[src], got_slots.at[g * members + src], s_send.at[step], s_recv.at[step],
            device_id={"mem": src},
        )

    def to_member(step):
        peer = target(m, step, members)
        return pltpu.make_async_remote_copy(
            vals.at[peer], got.at[mine], v_send.at[step], v_recv.at[step],
            device_id={"mem": peer},
        )

    def from_member(step):
        src = origin(m, step, members)
        return pltpu.make_async_remote_copy(
            vals.at[src], got.at[g * members + src], v_send.at[step], v_recv.at[step],
            device_id={"mem": src},
        )

    def to_group(step, hop):
        at = g * members + origin(m, step, members)
        return pltpu.make_async_remote_copy(
            got.at[at], got.at[at], f_send.at[step, hop], f_recv.at[step, hop],
            device_id={"grp": target(g, hop, groups)},
        )

    def from_group(step, hop):
        peer = origin(g, hop, groups)
        at = peer * members + origin(m, step, members)
        return pltpu.make_async_remote_copy(
            got.at[at], got.at[at], f_send.at[step, hop], f_recv.at[step, hop],
            device_id={"grp": peer},
        )

    def slots_to_group(hop):
        at = pl.ds(g * members, members)
        return pltpu.make_async_remote_copy(
            got_slots.at[at], got_slots.at[at], fs_send.at[hop], fs_recv.at[hop],
            device_id={"grp": target(g, hop, groups)},
        )

    def slots_from_group(hop):
        peer = origin(g, hop, groups)
        at = pl.ds(peer * members, members)
        return pltpu.make_async_remote_copy(
            got_slots.at[at], got_slots.at[at], fs_send.at[hop], fs_recv.at[hop],
            device_id={"grp": peer},
        )

    local_v = pltpu.make_async_copy(vals.at[m], got.at[mine], local_sem.at[0])
    local_s = pltpu.make_async_copy(own_slots.at[m], got_slots.at[mine], local_sem.at[2])
    local_v.start()
    local_s.start()
    each(1, members, lambda step: slots_to(step).start())
    each(1, members, lambda step: to_member(step).start())
    local_v.wait()
    local_s.wait()

    def forward(step):
        for hop in range(1, groups):
            to_group(step, hop).start()

    forward(0)

    def pass_on(step):
        from_member(step).wait_recv()
        forward(step)

    early = members - members // 4
    each(1, early, pass_on)
    each(1, members, lambda step: slots_from(step).wait_recv())
    for hop in range(1, groups):
        slots_to_group(hop).start()
    each(early, members, pass_on)
    for hop in range(1, groups):
        slots_from_group(hop).wait_recv()

    lane = lax.broadcasted_iota(jnp.int32, (1, LANES), 1)

    def pack(k):
        row = got_slots[k * per_row]
        for q in range(1, per_row):
            row = jnp.where(lane >= q * cap, got_slots[k * per_row + q], row)
        lane_i[pl.ds(k, 1), :] = jnp.where(row < 0, BUCKET, row)
        lane_f[pl.ds(k, 1), :] = row.astype(jnp.float32)

    each(0, total // LANES, pack)
    store_lane = pltpu.make_async_copy(lane_i, lane_ref, local_sem.at[1])
    store_lane.start()

    wide = min(WIDE, total)
    senders_wide = wide // cap
    halves = ROWS // LANES

    def column_of(b):
        columns = []
        for h in range(halves):
            row = lane_f[pl.ds(b * halves + h, 1), :]
            row = jnp.where(row < 0, -2.0, row)
            columns.append(jnp.transpose(jnp.broadcast_to(row, (LANES, LANES))))
        return jnp.concatenate(columns, axis=0)

    def same_part(column, w):
        same = []
        for l in range(wide // LANES):
            row = lane_f[pl.ds(w * (wide // LANES) + l, 1), :]
            same.append(jnp.where(column == row, 1.0, 0.0).astype(jnp.bfloat16))
        return jnp.concatenate(same, axis=1)

    def sum_part(same, w):
        rows = got[pl.ds(w * senders_wide, senders_wide)].reshape(wide, LANES)
        rows = jnp.concatenate([rows, jnp.ones((wide, LANES), jnp.bfloat16)], axis=1)
        return jnp.dot(same, rows, preferred_element_type=jnp.float32)

    def average(b, same_of):
        if total == wide:
            acc = sum_part(same_of(0), 0)
        else:
            acc = lax.fori_loop(
                0, total // wide, lambda w, a: a + sum_part(same_of(w), w),
                jnp.zeros((ROWS, 2 * LANES), jnp.float32),
            )
        avg = acc[:, :LANES] / jnp.maximum(acc[:, LANES:], 1.0)
        avg_v[pl.ds(b * ROWS, ROWS), :] = avg
        return avg

    def block(b):
        column = column_of(b)
        return average(b, lambda w: same_part(column, w))

    def store_avg(q):
        at = pl.ds(lax.rem(g + q, groups) * members * cap, members * cap)
        return pltpu.make_async_copy(avg_v.at[at], avg_ref.at[at], avg_sem.at[q])

    blocks_each = members * cap // ROWS
    senders_each = ROWS // cap

    held = blocks_each == 1 and total == wide
    if held:
        same_v[...] = same_part(column_of(g), 0)

    def land(step):
        for hop in range(1, groups):
            from_group(step, hop).wait_recv()

    each(0, members, land)

    def own_block(t):
        b = g * blocks_each + t
        avg = average(b, lambda w: same_v[...]) if held else block(b)
        ret[pl.ds(t * senders_each, senders_each)] = avg.astype(jnp.bfloat16).reshape(
            senders_each, cap, LANES
        )

    each(0, blocks_each, own_block)

    def back_to(step):
        peer = target(m, step, members)
        return pltpu.make_async_remote_copy(
            ret.at[peer], back_ref.at[m], r_send.at[step], r_recv.at[step],
            device_id={"mem": peer},
        )

    def back_from(step):
        src = origin(m, step, members)
        return pltpu.make_async_remote_copy(
            ret.at[src], back_ref.at[src], r_send.at[step], r_recv.at[step],
            device_id={"mem": src},
        )

    each(1, members, lambda step: back_to(members - step).start())
    local_r = pltpu.make_async_copy(ret.at[m], back_ref.at[m], local_sem.at[2])
    local_r.start()
    store_avg(0).start()

    for q in range(1, groups):
        other = lax.rem(g + q, groups)
        each(0, blocks_each, lambda t, other=other: (block(other * blocks_each + t), None)[1])
        store_avg(q).start()

    def finish_forward(step):
        for hop in range(1, groups):
            to_group(step, hop).wait_send()

    each(0, members, finish_forward)
    each(1, members, lambda step: (to_member(step).wait_send(), slots_to(step).wait_send())[0])
    for hop in range(1, groups):
        slots_to_group(hop).wait_send()
    store_lane.wait()
    for q in range(groups):
        store_avg(q).wait()
    local_r.wait()
    each(1, members, lambda step: back_to(step).wait_send())
    each(1, members, lambda step: back_from(step).wait_recv())


def place_kernel(total, avg_ref, slot_ref, back_ref, out_ref, returned_ref, table, rows, slot_s, back_v, in_sem, sems):
    unroll = 32
    load_s = pltpu.make_async_copy(slot_ref, slot_s, in_sem.at[0])
    load_a = pltpu.make_async_copy(avg_ref, rows, in_sem.at[1])
    load_b = pltpu.make_async_copy(back_ref, back_v, in_sem.at[2])
    store_b = pltpu.make_async_copy(back_v, returned_ref, in_sem.at[3])
    load_s.start()
    load_a.start()
    load_b.start()
    table[...] = jnp.zeros_like(table)
    load_s.wait()
    load_a.wait()
    load_b.wait()
    store_b.start()

    def step(i, carry):
        base = pl.multiple_of(i * unroll, unroll)
        row = base // LANES
        col = lax.rem(base, LANES)
        for k in range(unroll):
            s = slot_s[row, col + k]
            table[pl.ds(s, 1), :] = rows[pl.ds(base + k, 1), :]
        return carry

    lax.fori_loop(0, total // unroll, step, 0)
    pieces = sems.shape[0]
    size = BUCKET // pieces
    copies = [
        pltpu.make_async_copy(
            table.at[pl.ds(k * size, size)], out_ref.at[pl.ds(k * size, size)], sems.at[k]
        )
        for k in range(pieces)
    ]
    for copy in copies:
        copy.start()
    store_b.wait()
    for copy in copies:
        copy.wait()


def per_device(groups, members, values, slots, counts):
    cap, lanes = values.shape[2:]
    total = groups * members * cap
    hbm = pl.BlockSpec(memory_space=pl.ANY)
    dma = pltpu.SemaphoreType.DMA
    avg, lane_slots, back = pl.pallas_call(
        functools.partial(exchange_kernel, groups, members, cap),
        out_shape=(
            jax.ShapeDtypeStruct((total, lanes), jnp.float32),
            jax.ShapeDtypeStruct((total // LANES, LANES), jnp.int32),
            jax.ShapeDtypeStruct((members, cap, lanes), jnp.bfloat16),
        ),
        in_specs=[hbm, hbm, hbm],
        out_specs=(hbm, hbm, hbm),
        scratch_shapes=[
            pltpu.VMEM((groups * members, cap, lanes), jnp.bfloat16),
            pltpu.VMEM((groups * members, 1, LANES), jnp.int32),
            pltpu.VMEM((members, cap, lanes), jnp.bfloat16),
            pltpu.VMEM((members, 1, LANES), jnp.int32),
            pltpu.VMEM((members, cap), jnp.int32),
            pltpu.SMEM((1, members), jnp.int32),
            pltpu.VMEM((total // LANES, LANES), jnp.int32),
            pltpu.VMEM((total // LANES, LANES), jnp.float32),
            pltpu.VMEM((ROWS, min(WIDE, total)), jnp.bfloat16),
            pltpu.VMEM((total, lanes), jnp.float32),
            pltpu.VMEM((members, cap, lanes), jnp.bfloat16),
            dma((members,)), dma((members,)), dma((members,)), dma((members,)),
            dma((members, groups)), dma((members, groups)), dma((groups,)), dma((groups,)),
            dma((members,)), dma((members,)), dma((3,)), dma((groups,)),
        ],
        compiler_params=pltpu.CompilerParams(collective_id=0, has_side_effects=True),
    )(values, slots, counts)
    averaged, returned = pl.pallas_call(
        functools.partial(place_kernel, total),
        out_shape=(
            jax.ShapeDtypeStruct((BUCKET, lanes), jnp.float32),
            jax.ShapeDtypeStruct((members, cap, lanes), jnp.bfloat16),
        ),
        in_specs=[hbm, hbm, hbm],
        out_specs=(hbm, hbm),
        scratch_shapes=[
            pltpu.VMEM((BUCKET + 8, lanes), jnp.float32),
            pltpu.VMEM((total, lanes), jnp.float32),
            pltpu.SMEM((total // LANES, LANES), jnp.int32),
            pltpu.VMEM((members, cap, lanes), jnp.bfloat16),
            dma((4,)), dma((8,)),
        ],
    )(avg, lane_slots, back)
    return averaged, returned[None]


def solution(mesh):
    return jax.shard_map(
        functools.partial(per_device, mesh.shape["grp"], mesh.shape["mem"]),
        mesh=mesh,
        in_specs=(
            P(("grp", "mem"), None, None, None),
            P(("grp", "mem"), None, None),
            P(("grp", "mem"), None),
        ),
        out_specs=(P("mem", None), P(("grp", "mem"), None, None, None)),
        check_vma=False,
    )
```

```python
import functools

import jax
import jax.numpy as jnp
from jax import lax
from jax.experimental import pallas as pl
from jax.experimental.pallas import tpu as pltpu
from jax.sharding import PartitionSpec as P

BUCKET = 7168
LANES = 128
ROWS = 256
WIDE = 1024


def partner(index, step, count):
    if count & (count - 1):
        return None
    bit = 1
    while bit < count:
        flip = (step // bit) % 2
        index = index + flip * bit * (1 - 2 * ((index // bit) % 2))
        bit *= 2
    return index


def target(index, step, count):
    paired = partner(index, step, count)
    return lax.rem(index + step, count) if paired is None else paired


def origin(index, step, count):
    paired = partner(index, step, count)
    return lax.rem(index + count - step, count) if paired is None else paired


def exchange_kernel(
    groups, members, cap,
    values_ref, slots_ref, counts_ref,
    avg_ref, lane_ref, back_ref,
    got, got_slots, vals, own_slots, slots_v, counts_s, lane_i, lane_f, full_f, rank_f, halves_v, same_v, avg_v, ret,
    v_send, v_recv, s_send, s_recv, f_send, f_recv, fs_send, fs_recv,
    r_send, r_recv, local_sem, avg_sem,
):
    g = lax.axis_index("grp")
    m = lax.axis_index("mem")
    total = groups * members * cap
    per_row = LANES // cap

    def each(low, high, body):
        if high - low <= 8:
            for k in range(low, high):
                body(k)
        else:
            lax.fori_loop(low, high, lambda k, c: (body(k), c)[1], 0)

    barrier = pltpu.get_barrier_semaphore()
    for step in range(1, members):
        pl.semaphore_signal(barrier, inc=1, device_id={"mem": lax.rem(m + step, members)})
    for step in range(1, groups):
        pl.semaphore_signal(barrier, inc=1, device_id={"grp": lax.rem(g + step, groups)})

    load_v = pltpu.make_async_copy(values_ref.at[0], vals, local_sem.at[0])
    load_s = pltpu.make_async_copy(slots_ref.at[0], slots_v, local_sem.at[1])
    load_c = pltpu.make_async_copy(counts_ref, counts_s, local_sem.at[2])
    load_c.start()
    load_s.start()
    load_v.start()
    load_c.wait()
    load_s.wait()

    raw = slots_v[...]
    shown = jnp.concatenate([raw] * per_row, axis=1)
    row_id = lax.broadcasted_iota(jnp.int32, (members, LANES), 0)
    entry = lax.rem(lax.broadcasted_iota(jnp.int32, (members, LANES), 1), cap)
    limit = jnp.zeros((members, LANES), jnp.int32)
    for k in range(members):
        limit = jnp.where(row_id == k, counts_s[0, k], limit)
    masked = jnp.where(entry < limit, shown, -1)
    for k in range(members):
        own_slots[k] = masked[k : k + 1, :]
    load_v.wait()

    pl.semaphore_wait(barrier, members - 1 + groups - 1)

    mine = g * members + m

    def slots_to(step):
        peer = target(m, step, members)
        return pltpu.make_async_remote_copy(
            own_slots.at[peer], got_slots.at[mine], s_send.at[step], s_recv.at[step],
            device_id={"mem": peer},
        )

    def slots_from(step):
        src = origin(m, step, members)
        return pltpu.make_async_remote_copy(
            own_slots.at[src], got_slots.at[g * members + src], s_send.at[step], s_recv.at[step],
            device_id={"mem": src},
        )

    def to_member(step):
        peer = target(m, step, members)
        return pltpu.make_async_remote_copy(
            vals.at[peer], got.at[mine], v_send.at[step], v_recv.at[step],
            device_id={"mem": peer},
        )

    def from_member(step):
        src = origin(m, step, members)
        return pltpu.make_async_remote_copy(
            vals.at[src], got.at[g * members + src], v_send.at[step], v_recv.at[step],
            device_id={"mem": src},
        )

    def to_group(step, hop):
        at = g * members + origin(m, step, members)
        return pltpu.make_async_remote_copy(
            got.at[at], got.at[at], f_send.at[step, hop], f_recv.at[step, hop],
            device_id={"grp": target(g, hop, groups)},
        )

    def from_group(step, hop):
        peer = origin(g, hop, groups)
        at = peer * members + origin(m, step, members)
        return pltpu.make_async_remote_copy(
            got.at[at], got.at[at], f_send.at[step, hop], f_recv.at[step, hop],
            device_id={"grp": peer},
        )

    def slots_to_group(hop):
        at = pl.ds(g * members, members)
        return pltpu.make_async_remote_copy(
            got_slots.at[at], got_slots.at[at], fs_send.at[hop], fs_recv.at[hop],
            device_id={"grp": target(g, hop, groups)},
        )

    def slots_from_group(hop):
        peer = origin(g, hop, groups)
        at = pl.ds(peer * members, members)
        return pltpu.make_async_remote_copy(
            got_slots.at[at], got_slots.at[at], fs_send.at[hop], fs_recv.at[hop],
            device_id={"grp": peer},
        )

    local_v = pltpu.make_async_copy(vals.at[m], got.at[mine], local_sem.at[0])
    local_s = pltpu.make_async_copy(own_slots.at[m], got_slots.at[mine], local_sem.at[2])
    local_v.start()
    local_s.start()
    each(1, members, lambda step: slots_to(step).start())
    each(1, members, lambda step: to_member(step).start())
    local_v.wait()
    local_s.wait()

    def forward(step):
        for hop in range(1, groups):
            to_group(step, hop).start()

    forward(0)

    def pass_on(step):
        from_member(step).wait_recv()
        forward(step)

    early = members - members // 4
    each(1, early, pass_on)
    each(1, members, lambda step: slots_from(step).wait_recv())
    for hop in range(1, groups):
        slots_to_group(hop).start()
    each(early, members, pass_on)
    for hop in range(1, groups):
        slots_from_group(hop).wait_recv()

    lane = lax.broadcasted_iota(jnp.int32, (1, LANES), 1)

    def pack(k):
        row = got_slots[k * per_row]
        for q in range(1, per_row):
            row = jnp.where(lane >= q * cap, got_slots[k * per_row + q], row)
        lane_f[pl.ds(k, 1), :] = row.astype(jnp.float32)
        full_f[pl.ds(k, 1), :] = jnp.where(row < 0, BUCKET, row).astype(jnp.float32)

    each(0, total // LANES, pack)
    store_lane = pltpu.make_async_copy(lane_i, lane_ref, local_sem.at[1])

    wide = min(WIDE, total)
    senders_wide = wide // cap
    halves = ROWS // LANES

    def column_of(b):
        columns = []
        for h in range(halves):
            row = full_f[pl.ds(b * halves + h, 1), :]
            columns.append(jnp.transpose(jnp.broadcast_to(row, (LANES, LANES))))
        return jnp.concatenate(columns, axis=0)

    def same_part(column, w):
        same = []
        for l in range(wide // LANES):
            row = lane_f[pl.ds(w * (wide // LANES) + l, 1), :]
            same.append(jnp.where(column == row, 1.0, 0.0).astype(jnp.bfloat16))
        return jnp.concatenate(same, axis=1)

    def sum_part(same, w):
        rows = got[pl.ds(w * senders_wide, senders_wide)].reshape(wide, LANES)
        rows = jnp.concatenate([rows, jnp.ones((wide, LANES), jnp.bfloat16)], axis=1)
        return jnp.dot(same, rows, preferred_element_type=jnp.float32)

    def average(same_of):
        if total == wide:
            acc = sum_part(same_of(0), 0)
        else:
            acc = lax.fori_loop(
                0, total // wide, lambda w, a: a + sum_part(same_of(w), w),
                jnp.zeros((ROWS, 2 * LANES), jnp.float32),
            )
        return acc[:, :LANES] / jnp.maximum(acc[:, LANES:], 1.0)

    def block(b):
        column = column_of(b)
        return average(lambda w: same_part(column, w))

    blocks = total // ROWS

    def store_avg(b):
        at = pl.ds(b * ROWS, ROWS)
        return pltpu.make_async_copy(avg_v.at[at], avg_ref.at[at], avg_sem.at[b])

    blocks_each = members * cap // ROWS
    senders_each = ROWS // cap

    held = blocks_each == 1 and total == wide
    if held:
        same_v[...] = same_part(column_of(g), 0)

    def land(step):
        for hop in range(1, groups):
            from_group(step, hop).wait_recv()

    each(0, members, land)

    def own_block(t):
        b = g * blocks_each + t
        avg = average(lambda w: same_v[...]) if held else block(b)
        ret[pl.ds(t * senders_each, senders_each)] = avg.astype(jnp.bfloat16).reshape(
            senders_each, cap, LANES
        )

    each(0, blocks_each, own_block)

    def back_to(step):
        peer = target(m, step, members)
        return pltpu.make_async_remote_copy(
            ret.at[peer], back_ref.at[m], r_send.at[step], r_recv.at[step],
            device_id={"mem": peer},
        )

    def back_from(step):
        src = origin(m, step, members)
        return pltpu.make_async_remote_copy(
            ret.at[src], back_ref.at[src], r_send.at[step], r_recv.at[step],
            device_id={"mem": src},
        )

    each(1, members, lambda step: back_to(members - step).start())
    local_r = pltpu.make_async_copy(ret.at[m], back_ref.at[m], local_sem.at[2])
    local_r.start()

    def lay(b):
        column = column_of(b)
        high = jnp.floor(column * (1.0 / LANES))
        both = jnp.concatenate([high, column - high * LANES], axis=1)
        halves_v[pl.ds(b * ROWS, ROWS), :] = both.astype(jnp.bfloat16)

    each(0, blocks, lay)
    lines = wide // LANES
    down = lax.broadcasted_iota(jnp.int32, (ROWS, LANES), 0)

    def rank(w):
        keys = [
            full_f[pl.ds(w * lines + l, 1), :].astype(jnp.int32) * total + (w * lines + l) * LANES + lane
            for l in range(lines)
        ]

        def add(b, acc):
            both = halves_v[pl.ds(b * ROWS, ROWS), :].astype(jnp.float32)
            column = (both[:, :LANES] * float(LANES) + both[:, LANES:]).astype(jnp.int32)
            column = column * total + (b * ROWS + down)
            return tuple(
                a + jnp.sum(jnp.where(column < key, 1.0, 0.0), axis=0, keepdims=True)
                for a, key in zip(acc, keys)
            )

        acc = tuple(jnp.zeros((1, LANES), jnp.float32) for _ in range(lines))
        if blocks <= 8:
            for b in range(blocks):
                acc = add(b, acc)
        else:
            acc = lax.fori_loop(0, blocks, add, acc)
        for l in range(lines):
            rank_f[pl.ds(w * lines + l, 1), :] = acc[l]

    each(0, total // wide, rank)

    def ordered(b):
        place = (b * ROWS + down).astype(jnp.float32)

        def pick(w):
            chosen = jnp.concatenate(
                [
                    jnp.where(place == rank_f[pl.ds(w * lines + l, 1), :], 1.0, 0.0).astype(jnp.bfloat16)
                    for l in range(lines)
                ],
                axis=1,
            )
            return jnp.dot(
                chosen, halves_v[pl.ds(w * wide, wide), :], preferred_element_type=jnp.float32
            )

        if total == wide:
            acc = pick(0)
        else:
            acc = lax.fori_loop(
                0, total // wide, lambda w, a: a + pick(w), jnp.zeros((ROWS, 2 * LANES), jnp.float32)
            )
        column = acc[:, :LANES] * float(LANES) + acc[:, LANES:]
        for h in range(halves):
            turned = jnp.transpose(column[h * LANES : (h + 1) * LANES, :])
            lane_i[pl.ds(b * halves + h, 1), :] = turned[0:1, :].astype(jnp.int32)
        avg_v[pl.ds(b * ROWS, ROWS), :] = average(lambda w: same_part(column, w))
        store_avg(b).start()

    each(0, blocks, ordered)
    store_lane.start()

    def finish_forward(step):
        for hop in range(1, groups):
            to_group(step, hop).wait_send()

    each(0, members, finish_forward)
    each(1, members, lambda step: (to_member(step).wait_send(), slots_to(step).wait_send())[0])
    for hop in range(1, groups):
        slots_to_group(hop).wait_send()
    store_lane.wait()
    each(0, blocks, lambda b: store_avg(b).wait())
    local_r.wait()
    each(1, members, lambda step: back_to(step).wait_send())
    each(1, members, lambda step: back_from(step).wait_recv())


def place_kernel(total, avg_ref, slot_ref, back_ref, out_ref, returned_ref, table, rows, slot_s, back_v, in_sem, sems):
    unroll = 32
    load_s = pltpu.make_async_copy(slot_ref, slot_s, in_sem.at[0])
    load_a = pltpu.make_async_copy(avg_ref, rows, in_sem.at[1])
    load_b = pltpu.make_async_copy(back_ref, back_v, in_sem.at[2])
    store_b = pltpu.make_async_copy(back_v, returned_ref, in_sem.at[3])
    load_s.start()
    load_a.start()
    load_b.start()
    table[...] = jnp.zeros_like(table)
    load_s.wait()
    load_a.wait()
    load_b.wait()
    store_b.start()

    chunks = total // unroll
    pieces = sems.shape[0]
    size = BUCKET // pieces

    def more(bound, i):
        at = jnp.minimum(i, chunks - 1) * unroll
        return jnp.logical_and(i < chunks, slot_s[at // LANES, lax.rem(at, LANES)] < bound)

    def step(i):
        base = pl.multiple_of(i * unroll, unroll)
        row = base // LANES
        col = lax.rem(base, LANES)
        for k in range(unroll):
            s = slot_s[row, col + k]
            table[pl.ds(s, 1), :] = rows[pl.ds(base + k, 1), :]
        return i + 1

    copies = []
    at = jnp.int32(0)
    for k in range(pieces):
        at = lax.while_loop(functools.partial(more, (k + 1) * size), step, at)
        copy = pltpu.make_async_copy(
            table.at[pl.ds(k * size, size)], out_ref.at[pl.ds(k * size, size)], sems.at[k]
        )
        copy.start()
        copies.append(copy)
    store_b.wait()
    for copy in copies:
        copy.wait()


def per_device(groups, members, values, slots, counts):
    cap, lanes = values.shape[2:]
    total = groups * members * cap
    hbm = pl.BlockSpec(memory_space=pl.ANY)
    dma = pltpu.SemaphoreType.DMA
    avg, lane_slots, back = pl.pallas_call(
        functools.partial(exchange_kernel, groups, members, cap),
        out_shape=(
            jax.ShapeDtypeStruct((total, lanes), jnp.float32),
            jax.ShapeDtypeStruct((total // LANES, LANES), jnp.int32),
            jax.ShapeDtypeStruct((members, cap, lanes), jnp.bfloat16),
        ),
        in_specs=[hbm, hbm, hbm],
        out_specs=(hbm, hbm, hbm),
        scratch_shapes=[
            pltpu.VMEM((groups * members, cap, lanes), jnp.bfloat16),
            pltpu.VMEM((groups * members, 1, LANES), jnp.int32),
            pltpu.VMEM((members, cap, lanes), jnp.bfloat16),
            pltpu.VMEM((members, 1, LANES), jnp.int32),
            pltpu.VMEM((members, cap), jnp.int32),
            pltpu.SMEM((1, members), jnp.int32),
            pltpu.VMEM((total // LANES, LANES), jnp.int32),
            pltpu.VMEM((total // LANES, LANES), jnp.float32),
            pltpu.VMEM((total // LANES, LANES), jnp.float32),
            pltpu.VMEM((total // LANES, LANES), jnp.float32),
            pltpu.VMEM((total, 2 * LANES), jnp.bfloat16),
            pltpu.VMEM((ROWS, min(WIDE, total)), jnp.bfloat16),
            pltpu.VMEM((total, lanes), jnp.float32),
            pltpu.VMEM((members, cap, lanes), jnp.bfloat16),
            dma((members,)), dma((members,)), dma((members,)), dma((members,)),
            dma((members, groups)), dma((members, groups)), dma((groups,)), dma((groups,)),
            dma((members,)), dma((members,)), dma((3,)), dma((total // ROWS,)),
        ],
        compiler_params=pltpu.CompilerParams(collective_id=0, has_side_effects=True),
    )(values, slots, counts)
    averaged, returned = pl.pallas_call(
        functools.partial(place_kernel, total),
        out_shape=(
            jax.ShapeDtypeStruct((BUCKET, lanes), jnp.float32),
            jax.ShapeDtypeStruct((members, cap, lanes), jnp.bfloat16),
        ),
        in_specs=[hbm, hbm, hbm],
        out_specs=(hbm, hbm),
        scratch_shapes=[
            pltpu.VMEM((BUCKET + 8, lanes), jnp.float32),
            pltpu.VMEM((total, lanes), jnp.float32),
            pltpu.SMEM((total // LANES, LANES), jnp.int32),
            pltpu.VMEM((members, cap, lanes), jnp.bfloat16),
            dma((4,)), dma((8,)),
        ],
    )(avg, lane_slots, back)
    return averaged, returned[None]


def solution(mesh):
    return jax.shard_map(
        functools.partial(per_device, mesh.shape["grp"], mesh.shape["mem"]),
        mesh=mesh,
        in_specs=(
            P(("grp", "mem"), None, None, None),
            P(("grp", "mem"), None, None),
            P(("grp", "mem"), None),
        ),
        out_specs=(P("mem", None), P(("grp", "mem"), None, None, None)),
        check_vma=False,
    )
```

```python
import functools

import jax
import jax.numpy as jnp
from jax import lax
from jax.experimental import pallas as pl
from jax.experimental.pallas import tpu as pltpu
from jax.sharding import PartitionSpec as P

BUCKET = 7168
LANES = 128
ROWS = 256
WIDE = 1024
JOINED = 2


def partner(index, step, count):
    if count & (count - 1):
        return None
    bit = 1
    while bit < count:
        flip = (step // bit) % 2
        index = index + flip * bit * (1 - 2 * ((index // bit) % 2))
        bit *= 2
    return index


def target(index, step, count):
    paired = partner(index, step, count)
    return lax.rem(index + step, count) if paired is None else paired


def origin(index, step, count):
    paired = partner(index, step, count)
    return lax.rem(index + count - step, count) if paired is None else paired


def exchange_kernel(
    groups, members, cap,
    values_ref, slots_ref, counts_ref,
    avg_ref, lane_ref, back_ref,
    got, got_slots, vals, own_slots, slots_v, counts_s, lane_i, lane_f, full_f, rank_f, halves_v, same_v, avg_v, ret,
    v_send, v_recv, s_send, s_recv, f_send, f_recv, fs_send, fs_recv,
    r_send, r_recv, local_sem, avg_sem,
):
    g = lax.axis_index("grp")
    m = lax.axis_index("mem")
    total = groups * members * cap
    per_row = LANES // cap
    joined = 1 if members & (members - 1) else min(members, JOINED)

    def each(low, high, body):
        if high - low <= 8:
            for k in range(low, high):
                body(k)
        else:
            lax.fori_loop(low, high, lambda k, c: (body(k), c)[1], 0)

    barrier = pltpu.get_barrier_semaphore()
    for step in range(1, members):
        pl.semaphore_signal(barrier, inc=1, device_id={"mem": lax.rem(m + step, members)})
    for step in range(1, groups):
        pl.semaphore_signal(barrier, inc=1, device_id={"grp": lax.rem(g + step, groups)})

    load_v = pltpu.make_async_copy(values_ref.at[0], vals, local_sem.at[0])
    load_s = pltpu.make_async_copy(slots_ref.at[0], slots_v, local_sem.at[1])
    load_c = pltpu.make_async_copy(counts_ref, counts_s, local_sem.at[2])
    load_c.start()
    load_s.start()
    load_v.start()
    load_c.wait()
    load_s.wait()

    raw = slots_v[...]
    shown = jnp.concatenate([raw] * per_row, axis=1)
    row_id = lax.broadcasted_iota(jnp.int32, (members, LANES), 0)
    entry = lax.rem(lax.broadcasted_iota(jnp.int32, (members, LANES), 1), cap)
    limit = jnp.zeros((members, LANES), jnp.int32)
    for k in range(members):
        limit = jnp.where(row_id == k, counts_s[0, k], limit)
    masked = jnp.where(entry < limit, shown, -1)
    for k in range(members):
        own_slots[k] = masked[k : k + 1, :]
    load_v.wait()

    pl.semaphore_wait(barrier, members - 1 + groups - 1)

    mine = g * members + m

    def slots_to(step):
        peer = target(m, step, members)
        return pltpu.make_async_remote_copy(
            own_slots.at[peer], got_slots.at[mine], s_send.at[step], s_recv.at[step],
            device_id={"mem": peer},
        )

    def slots_from(step):
        src = origin(m, step, members)
        return pltpu.make_async_remote_copy(
            own_slots.at[src], got_slots.at[g * members + src], s_send.at[step], s_recv.at[step],
            device_id={"mem": src},
        )

    def to_member(step):
        peer = target(m, step, members)
        return pltpu.make_async_remote_copy(
            vals.at[peer], got.at[mine], v_send.at[step], v_recv.at[step],
            device_id={"mem": peer},
        )

    def from_member(step):
        src = origin(m, step, members)
        return pltpu.make_async_remote_copy(
            vals.at[src], got.at[g * members + src], v_send.at[step], v_recv.at[step],
            device_id={"mem": src},
        )

    def to_group(step, hop):
        at = pl.ds(g * members + origin(m - lax.rem(m, joined), step, members), joined)
        return pltpu.make_async_remote_copy(
            got.at[at], got.at[at], f_send.at[step, hop], f_recv.at[step, hop],
            device_id={"grp": target(g, hop, groups)},
        )

    def from_group(step, hop):
        peer = origin(g, hop, groups)
        at = pl.ds(peer * members + origin(m - lax.rem(m, joined), step, members), joined)
        return pltpu.make_async_remote_copy(
            got.at[at], got.at[at], f_send.at[step, hop], f_recv.at[step, hop],
            device_id={"grp": peer},
        )

    def slots_to_group(hop):
        at = pl.ds(g * members, members)
        return pltpu.make_async_remote_copy(
            got_slots.at[at], got_slots.at[at], fs_send.at[hop], fs_recv.at[hop],
            device_id={"grp": target(g, hop, groups)},
        )

    def slots_from_group(hop):
        peer = origin(g, hop, groups)
        at = pl.ds(peer * members, members)
        return pltpu.make_async_remote_copy(
            got_slots.at[at], got_slots.at[at], fs_send.at[hop], fs_recv.at[hop],
            device_id={"grp": peer},
        )

    local_v = pltpu.make_async_copy(vals.at[m], got.at[mine], local_sem.at[0])
    local_s = pltpu.make_async_copy(own_slots.at[m], got_slots.at[mine], local_sem.at[2])
    local_v.start()
    local_s.start()
    each(1, members, lambda step: slots_to(members - step).start())
    to_member(1).start()
    each(1, members - 1, lambda step: to_member(members - step).start())
    local_v.wait()
    local_s.wait()

    def forward(step):
        for hop in range(1, groups):
            to_group(step, hop).start()

    each(1, joined, lambda step: from_member(step).wait_recv())
    forward(0)

    def pass_on(turn):
        for k in range(joined):
            from_member(turn * joined + k).wait_recv()
        forward(turn * joined)

    turns = members // joined
    early = max(1, turns - max(1, turns // 4))
    each(1, early, pass_on)
    each(1, members, lambda step: slots_from(step).wait_recv())
    for hop in range(1, groups):
        slots_to_group(hop).start()
    each(early, turns, pass_on)
    for hop in range(1, groups):
        slots_from_group(hop).wait_recv()

    lane = lax.broadcasted_iota(jnp.int32, (1, LANES), 1)

    def pack(k):
        row = got_slots[k * per_row]
        for q in range(1, per_row):
            row = jnp.where(lane >= q * cap, got_slots[k * per_row + q], row)
        lane_f[pl.ds(k, 1), :] = row.astype(jnp.float32)
        full_f[pl.ds(k, 1), :] = jnp.where(row < 0, BUCKET, row).astype(jnp.float32)

    each(0, total // LANES, pack)
    store_lane = pltpu.make_async_copy(lane_i, lane_ref, local_sem.at[1])

    wide = min(WIDE, total)
    senders_wide = wide // cap
    halves = ROWS // LANES

    def column_of(b):
        columns = []
        for h in range(halves):
            row = full_f[pl.ds(b * halves + h, 1), :]
            columns.append(jnp.transpose(jnp.broadcast_to(row, (LANES, LANES))))
        return jnp.concatenate(columns, axis=0)

    def same_part(column, w):
        same = []
        for l in range(wide // LANES):
            row = lane_f[pl.ds(w * (wide // LANES) + l, 1), :]
            same.append(jnp.where(column == row, 1.0, 0.0).astype(jnp.bfloat16))
        return jnp.concatenate(same, axis=1)

    def sum_part(same, w):
        rows = got[pl.ds(w * senders_wide, senders_wide)].reshape(wide, LANES)
        rows = jnp.concatenate([rows, jnp.ones((wide, LANES), jnp.bfloat16)], axis=1)
        return jnp.dot(same, rows, preferred_element_type=jnp.float32)

    def average(same_of):
        if total == wide:
            acc = sum_part(same_of(0), 0)
        else:
            acc = lax.fori_loop(
                0, total // wide, lambda w, a: a + sum_part(same_of(w), w),
                jnp.zeros((ROWS, 2 * LANES), jnp.float32),
            )
        return acc[:, :LANES] / jnp.maximum(acc[:, LANES:], 1.0)

    def block(b):
        column = column_of(b)
        return average(lambda w: same_part(column, w))

    blocks = total // ROWS

    def store_avg(b):
        at = pl.ds(b * ROWS, ROWS)
        return pltpu.make_async_copy(avg_v.at[at], avg_ref.at[at], avg_sem.at[b])

    blocks_each = members * cap // ROWS
    senders_each = ROWS // cap

    held = blocks_each == 1 and total == wide
    if held:
        same_v[...] = same_part(column_of(g), 0)

    def land(step):
        for hop in range(1, groups):
            from_group(step * joined, hop).wait_recv()

    each(0, turns, land)

    def own_block(t):
        b = g * blocks_each + t
        avg = average(lambda w: same_v[...]) if held else block(b)
        ret[pl.ds(t * senders_each, senders_each)] = avg.astype(jnp.bfloat16).reshape(
            senders_each, cap, LANES
        )

    each(0, blocks_each, own_block)

    def back_to(step):
        peer = target(m, step, members)
        return pltpu.make_async_remote_copy(
            ret.at[peer], back_ref.at[m], r_send.at[step], r_recv.at[step],
            device_id={"mem": peer},
        )

    def back_from(step):
        src = origin(m, step, members)
        return pltpu.make_async_remote_copy(
            ret.at[src], back_ref.at[src], r_send.at[step], r_recv.at[step],
            device_id={"mem": src},
        )

    each(1, members, lambda step: back_to(members - step).start())
    local_r = pltpu.make_async_copy(ret.at[m], back_ref.at[m], local_sem.at[2])
    local_r.start()

    def lay(b):
        column = column_of(b)
        high = jnp.floor(column * (1.0 / LANES))
        both = jnp.concatenate([high, column - high * LANES], axis=1)
        halves_v[pl.ds(b * ROWS, ROWS), :] = both.astype(jnp.bfloat16)

    each(0, blocks, lay)
    lines = wide // LANES
    down = lax.broadcasted_iota(jnp.int32, (ROWS, LANES), 0)

    def rank(w):
        keys = [
            full_f[pl.ds(w * lines + l, 1), :].astype(jnp.int32) * total + (w * lines + l) * LANES + lane
            for l in range(lines)
        ]

        def add(b, acc):
            both = halves_v[pl.ds(b * ROWS, ROWS), :].astype(jnp.float32)
            column = (both[:, :LANES] * float(LANES) + both[:, LANES:]).astype(jnp.int32)
            column = column * total + (b * ROWS + down)
            return tuple(
                a + jnp.sum(jnp.where(column < key, 1.0, 0.0), axis=0, keepdims=True)
                for a, key in zip(acc, keys)
            )

        acc = tuple(jnp.zeros((1, LANES), jnp.float32) for _ in range(lines))
        if blocks <= 8:
            for b in range(blocks):
                acc = add(b, acc)
        else:
            acc = lax.fori_loop(0, blocks, add, acc)
        for l in range(lines):
            rank_f[pl.ds(w * lines + l, 1), :] = acc[l]

    each(0, total // wide, rank)

    def ordered(b):
        place = (b * ROWS + down).astype(jnp.float32)

        def pick(w):
            chosen = jnp.concatenate(
                [
                    jnp.where(place == rank_f[pl.ds(w * lines + l, 1), :], 1.0, 0.0).astype(jnp.bfloat16)
                    for l in range(lines)
                ],
                axis=1,
            )
            return jnp.dot(
                chosen, halves_v[pl.ds(w * wide, wide), :], preferred_element_type=jnp.float32
            )

        if total == wide:
            acc = pick(0)
        else:
            acc = lax.fori_loop(
                0, total // wide, lambda w, a: a + pick(w), jnp.zeros((ROWS, 2 * LANES), jnp.float32)
            )
        column = acc[:, :LANES] * float(LANES) + acc[:, LANES:]
        for h in range(halves):
            turned = jnp.transpose(column[h * LANES : (h + 1) * LANES, :])
            lane_i[pl.ds(b * halves + h, 1), :] = turned[0:1, :].astype(jnp.int32)
        avg_v[pl.ds(b * ROWS, ROWS), :] = average(lambda w: same_part(column, w))
        store_avg(b).start()

    each(0, blocks, ordered)
    store_lane.start()

    def finish_forward(step):
        for hop in range(1, groups):
            to_group(step * joined, hop).wait_send()

    each(0, turns, finish_forward)
    each(1, members, lambda step: (to_member(step).wait_send(), slots_to(step).wait_send())[0])
    for hop in range(1, groups):
        slots_to_group(hop).wait_send()
    store_lane.wait()
    each(0, blocks, lambda b: store_avg(b).wait())
    local_r.wait()
    each(1, members, lambda step: back_to(step).wait_send())
    each(1, members, lambda step: back_from(step).wait_recv())


def place_kernel(total, avg_ref, slot_ref, back_ref, out_ref, returned_ref, table, rows, slot_s, back_v, in_sem, sems):
    unroll = LANES
    load_s = pltpu.make_async_copy(slot_ref, slot_s, in_sem.at[0])
    load_a = pltpu.make_async_copy(avg_ref, rows, in_sem.at[1])
    load_b = pltpu.make_async_copy(back_ref, back_v, in_sem.at[2])
    store_b = pltpu.make_async_copy(back_v, returned_ref, in_sem.at[3])
    load_s.start()
    load_a.start()
    load_b.start()
    table[...] = jnp.zeros_like(table)
    load_s.wait()
    load_a.wait()
    load_b.wait()
    store_b.start()

    chunks = total // unroll
    pieces = sems.shape[0]
    size = BUCKET // pieces

    def more(bound, i):
        return jnp.logical_and(i < chunks, slot_s[jnp.minimum(i, chunks - 1), 0] < bound)

    def step(i):
        base = pl.multiple_of(i * unroll, unroll)
        for k in range(unroll):
            s = slot_s[i, k]
            table[pl.ds(s, 1), :] = rows[pl.ds(base + k, 1), :]
        return i + 1

    copies = []
    at = jnp.int32(0)
    for k in range(pieces):
        at = lax.while_loop(functools.partial(more, (k + 1) * size), step, at)
        copy = pltpu.make_async_copy(
            table.at[pl.ds(k * size, size)], out_ref.at[pl.ds(k * size, size)], sems.at[k]
        )
        copy.start()
        copies.append(copy)
    store_b.wait()
    for copy in copies:
        copy.wait()


def per_device(groups, members, values, slots, counts):
    cap, lanes = values.shape[2:]
    total = groups * members * cap
    hbm = pl.BlockSpec(memory_space=pl.ANY)
    dma = pltpu.SemaphoreType.DMA
    avg, lane_slots, back = pl.pallas_call(
        functools.partial(exchange_kernel, groups, members, cap),
        out_shape=(
            jax.ShapeDtypeStruct((total, lanes), jnp.float32),
            jax.ShapeDtypeStruct((total // LANES, LANES), jnp.int32),
            jax.ShapeDtypeStruct((members, cap, lanes), jnp.bfloat16),
        ),
        in_specs=[hbm, hbm, hbm],
        out_specs=(hbm, hbm, hbm),
        scratch_shapes=[
            pltpu.VMEM((groups * members, cap, lanes), jnp.bfloat16),
            pltpu.VMEM((groups * members, 1, LANES), jnp.int32),
            pltpu.VMEM((members, cap, lanes), jnp.bfloat16),
            pltpu.VMEM((members, 1, LANES), jnp.int32),
            pltpu.VMEM((members, cap), jnp.int32),
            pltpu.SMEM((1, members), jnp.int32),
            pltpu.VMEM((total // LANES, LANES), jnp.int32),
            pltpu.VMEM((total // LANES, LANES), jnp.float32),
            pltpu.VMEM((total // LANES, LANES), jnp.float32),
            pltpu.VMEM((total // LANES, LANES), jnp.float32),
            pltpu.VMEM((total, 2 * LANES), jnp.bfloat16),
            pltpu.VMEM((ROWS, min(WIDE, total)), jnp.bfloat16),
            pltpu.VMEM((total, lanes), jnp.float32),
            pltpu.VMEM((members, cap, lanes), jnp.bfloat16),
            dma((members,)), dma((members,)), dma((members,)), dma((members,)),
            dma((members, groups)), dma((members, groups)), dma((groups,)), dma((groups,)),
            dma((members,)), dma((members,)), dma((3,)), dma((total // ROWS,)),
        ],
        compiler_params=pltpu.CompilerParams(collective_id=0, has_side_effects=True),
    )(values, slots, counts)
    averaged, returned = pl.pallas_call(
        functools.partial(place_kernel, total),
        out_shape=(
            jax.ShapeDtypeStruct((BUCKET, lanes), jnp.float32),
            jax.ShapeDtypeStruct((members, cap, lanes), jnp.bfloat16),
        ),
        in_specs=[hbm, hbm, hbm],
        out_specs=(hbm, hbm),
        scratch_shapes=[
            pltpu.VMEM((BUCKET + 8, lanes), jnp.float32),
            pltpu.VMEM((total, lanes), jnp.float32),
            pltpu.SMEM((total // LANES, LANES), jnp.int32),
            pltpu.VMEM((members, cap, lanes), jnp.bfloat16),
            dma((4,)), dma((8,)),
        ],
    )(avg, lane_slots, back)
    return averaged, returned[None]


def solution(mesh):
    return jax.shard_map(
        functools.partial(per_device, mesh.shape["grp"], mesh.shape["mem"]),
        mesh=mesh,
        in_specs=(
            P(("grp", "mem"), None, None, None),
            P(("grp", "mem"), None, None),
            P(("grp", "mem"), None),
        ),
        out_specs=(P("mem", None), P(("grp", "mem"), None, None, None)),
        check_vma=False,
    )
```

```python
import functools

import jax
import jax.numpy as jnp
from jax import lax
from jax.experimental import pallas as pl
from jax.experimental.pallas import tpu as pltpu
from jax.sharding import PartitionSpec as P

BUCKET = 7168
LANES = 128
ROWS = 256
WIDE = 1024
JOINED = 2


def partner(index, step, count):
    if count & (count - 1):
        return None
    bit = 1
    while bit < count:
        flip = (step // bit) % 2
        index = index + flip * bit * (1 - 2 * ((index // bit) % 2))
        bit *= 2
    return index


def target(index, step, count):
    paired = partner(index, step, count)
    return lax.rem(index + step, count) if paired is None else paired


def origin(index, step, count):
    paired = partner(index, step, count)
    return lax.rem(index + count - step, count) if paired is None else paired


def exchange_kernel(
    groups, members, cap,
    values_ref, slots_ref, counts_ref,
    avg_ref, lane_ref, back_ref,
    got, got_slots, vals, own_slots, slots_v, counts_s, lane_i, lane_f, full_f, rank_f, halves_v, same_v, avg_v, ret,
    v_send, v_recv, s_send, s_recv, f_send, f_recv, fs_send, fs_recv,
    r_send, r_recv, local_sem, avg_sem,
):
    g = lax.axis_index("grp")
    m = lax.axis_index("mem")
    total = groups * members * cap
    per_row = LANES // cap
    joined = 1 if members & (members - 1) else min(members, JOINED)

    def each(low, high, body):
        if high - low <= 8:
            for k in range(low, high):
                body(k)
        else:
            lax.fori_loop(low, high, lambda k, c: (body(k), c)[1], 0)

    barrier = pltpu.get_barrier_semaphore()
    for step in range(1, members):
        pl.semaphore_signal(barrier, inc=1, device_id={"mem": lax.rem(m + step, members)})
    for step in range(1, groups):
        pl.semaphore_signal(barrier, inc=1, device_id={"grp": lax.rem(g + step, groups)})

    load_v = pltpu.make_async_copy(values_ref.at[0], vals, local_sem.at[0])
    load_s = pltpu.make_async_copy(slots_ref.at[0], slots_v, local_sem.at[1])
    load_c = pltpu.make_async_copy(counts_ref, counts_s, local_sem.at[2])
    load_c.start()
    load_s.start()
    load_v.start()
    load_c.wait()
    load_s.wait()

    raw = slots_v[...]
    shown = jnp.concatenate([raw] * per_row, axis=1)
    row_id = lax.broadcasted_iota(jnp.int32, (members, LANES), 0)
    entry = lax.rem(lax.broadcasted_iota(jnp.int32, (members, LANES), 1), cap)
    limit = jnp.zeros((members, LANES), jnp.int32)
    for k in range(members):
        limit = jnp.where(row_id == k, counts_s[0, k], limit)
    masked = jnp.where(entry < limit, shown, -1)
    for k in range(members):
        own_slots[k] = masked[k : k + 1, :]
    load_v.wait()

    pl.semaphore_wait(barrier, members - 1 + groups - 1)

    mine = g * members + m

    def slots_to(step):
        peer = target(m, step, members)
        return pltpu.make_async_remote_copy(
            own_slots.at[peer], got_slots.at[mine], s_send.at[step], s_recv.at[step],
            device_id={"mem": peer},
        )

    def slots_from(step):
        src = origin(m, step, members)
        return pltpu.make_async_remote_copy(
            own_slots.at[src], got_slots.at[g * members + src], s_send.at[step], s_recv.at[step],
            device_id={"mem": src},
        )

    def to_member(step):
        peer = target(m, step, members)
        return pltpu.make_async_remote_copy(
            vals.at[peer], got.at[mine], v_send.at[step], v_recv.at[step],
            device_id={"mem": peer},
        )

    def from_member(step):
        src = origin(m, step, members)
        return pltpu.make_async_remote_copy(
            vals.at[src], got.at[g * members + src], v_send.at[step], v_recv.at[step],
            device_id={"mem": src},
        )

    def to_group(step, hop):
        at = pl.ds(g * members + origin(m - lax.rem(m, joined), step, members), joined)
        return pltpu.make_async_remote_copy(
            got.at[at], got.at[at], f_send.at[step, hop], f_recv.at[step, hop],
            device_id={"grp": target(g, hop, groups)},
        )

    def from_group(step, hop):
        peer = origin(g, hop, groups)
        at = pl.ds(peer * members + origin(m - lax.rem(m, joined), step, members), joined)
        return pltpu.make_async_remote_copy(
            got.at[at], got.at[at], f_send.at[step, hop], f_recv.at[step, hop],
            device_id={"grp": peer},
        )

    def slots_to_group(hop):
        at = pl.ds(g * members, members)
        return pltpu.make_async_remote_copy(
            got_slots.at[at], got_slots.at[at], fs_send.at[hop], fs_recv.at[hop],
            device_id={"grp": target(g, hop, groups)},
        )

    def slots_from_group(hop):
        peer = origin(g, hop, groups)
        at = pl.ds(peer * members, members)
        return pltpu.make_async_remote_copy(
            got_slots.at[at], got_slots.at[at], fs_send.at[hop], fs_recv.at[hop],
            device_id={"grp": peer},
        )

    local_v = pltpu.make_async_copy(vals.at[m], got.at[mine], local_sem.at[0])
    local_s = pltpu.make_async_copy(own_slots.at[m], got_slots.at[mine], local_sem.at[2])
    local_v.start()
    local_s.start()
    each(1, members, lambda step: slots_to(members - step).start())
    to_member(1).start()
    each(1, members - 1, lambda step: to_member(members - step).start())
    local_v.wait()
    local_s.wait()

    def forward(step):
        for hop in range(1, groups):
            to_group(step, hop).start()

    each(1, joined, lambda step: from_member(step).wait_recv())
    forward(0)

    def pass_on(turn):
        for k in range(joined):
            from_member(turn * joined + k).wait_recv()
        forward(turn * joined)

    turns = members // joined
    early = max(1, turns - max(1, turns // 4))
    each(1, early, pass_on)
    each(1, members, lambda step: slots_from(step).wait_recv())
    for hop in range(1, groups):
        slots_to_group(hop).start()
    each(early, turns, pass_on)
    for hop in range(1, groups):
        slots_from_group(hop).wait_recv()

    lane = lax.broadcasted_iota(jnp.int32, (1, LANES), 1)

    def pack(k):
        row = got_slots[k * per_row]
        for q in range(1, per_row):
            row = jnp.where(lane >= q * cap, got_slots[k * per_row + q], row)
        lane_f[pl.ds(k, 1), :] = row.astype(jnp.float32)
        full_f[pl.ds(k, 1), :] = jnp.where(row < 0, BUCKET, row).astype(jnp.float32)

    each(0, total // LANES, pack)
    store_lane = pltpu.make_async_copy(lane_i, lane_ref, local_sem.at[1])

    wide = min(WIDE, total)
    senders_wide = wide // cap
    halves = ROWS // LANES

    def column_of(b):
        columns = []
        for h in range(halves):
            row = full_f[pl.ds(b * halves + h, 1), :]
            columns.append(jnp.transpose(jnp.broadcast_to(row, (LANES, LANES))))
        return jnp.concatenate(columns, axis=0)

    def same_part(column, w):
        same = []
        for l in range(wide // LANES):
            row = lane_f[pl.ds(w * (wide // LANES) + l, 1), :]
            same.append(jnp.where(column == row, 1.0, 0.0).astype(jnp.bfloat16))
        return jnp.concatenate(same, axis=1)

    def sum_part(same, w):
        rows = got[pl.ds(w * senders_wide, senders_wide)].reshape(wide, LANES)
        rows = jnp.concatenate([rows, jnp.ones((wide, LANES), jnp.bfloat16)], axis=1)
        return jnp.dot(same, rows, preferred_element_type=jnp.float32)

    def average(same_of):
        if total == wide:
            acc = sum_part(same_of(0), 0)
        else:
            acc = lax.fori_loop(
                0, total // wide, lambda w, a: a + sum_part(same_of(w), w),
                jnp.zeros((ROWS, 2 * LANES), jnp.float32),
            )
        return acc[:, :LANES] / jnp.maximum(acc[:, LANES:], 1.0)

    def block(b):
        column = column_of(b)
        return average(lambda w: same_part(column, w))

    blocks = total // ROWS

    def store_avg(b):
        at = pl.ds(b * ROWS, ROWS)
        return pltpu.make_async_copy(avg_v.at[at], avg_ref.at[at], avg_sem.at[b])

    blocks_each = members * cap // ROWS
    senders_each = ROWS // cap

    held = blocks_each == 1 and total == wide
    if held:
        same_v[...] = same_part(column_of(g), 0)

    def land(step):
        for hop in range(1, groups):
            from_group(step * joined, hop).wait_recv()

    each(0, turns, land)

    def own_block(t):
        b = g * blocks_each + t
        avg = average(lambda w: same_v[...]) if held else block(b)
        ret[pl.ds(t * senders_each, senders_each)] = avg.astype(jnp.bfloat16).reshape(
            senders_each, cap, LANES
        )

    each(0, blocks_each, own_block)

    def back_to(step):
        peer = target(m, step, members)
        return pltpu.make_async_remote_copy(
            ret.at[peer], back_ref.at[m], r_send.at[step], r_recv.at[step],
            device_id={"mem": peer},
        )

    def back_from(step):
        src = origin(m, step, members)
        return pltpu.make_async_remote_copy(
            ret.at[src], back_ref.at[src], r_send.at[step], r_recv.at[step],
            device_id={"mem": src},
        )

    chips = members // 2
    if chips == 4:
        outer = jnp.where(lax.rem(m // 2 + 1, chips) < 2, 1, 0)
        for lo, hi in ((6, 4), (7, 5), (4, 6), (5, 7), (2, 2), (3, 3), (1, 1)):
            back_to(outer * lo + (1 - outer) * hi).start()
    else:
        each(1, members, lambda step: back_to(members - step).start())
    local_r = pltpu.make_async_copy(ret.at[m], back_ref.at[m], local_sem.at[2])
    local_r.start()

    def lay(b):
        column = column_of(b)
        high = jnp.floor(column * (1.0 / LANES))
        both = jnp.concatenate([high, column - high * LANES], axis=1)
        halves_v[pl.ds(b * ROWS, ROWS), :] = both.astype(jnp.bfloat16)

    each(0, blocks, lay)
    lines = wide // LANES
    down = lax.broadcasted_iota(jnp.int32, (ROWS, LANES), 0)

    def rank(w):
        keys = [
            full_f[pl.ds(w * lines + l, 1), :].astype(jnp.int32) * total + (w * lines + l) * LANES + lane
            for l in range(lines)
        ]

        def add(b, acc):
            both = halves_v[pl.ds(b * ROWS, ROWS), :].astype(jnp.float32)
            column = (both[:, :LANES] * float(LANES) + both[:, LANES:]).astype(jnp.int32)
            column = column * total + (b * ROWS + down)
            return tuple(
                a + jnp.sum(jnp.where(column < key, 1.0, 0.0), axis=0, keepdims=True)
                for a, key in zip(acc, keys)
            )

        acc = tuple(jnp.zeros((1, LANES), jnp.float32) for _ in range(lines))
        if blocks <= 8:
            for b in range(blocks):
                acc = add(b, acc)
        else:
            acc = lax.fori_loop(0, blocks, add, acc)
        for l in range(lines):
            rank_f[pl.ds(w * lines + l, 1), :] = acc[l]

    each(0, total // wide, rank)

    def ordered(b):
        place = (b * ROWS + down).astype(jnp.float32)

        def pick(w):
            chosen = jnp.concatenate(
                [
                    jnp.where(place == rank_f[pl.ds(w * lines + l, 1), :], 1.0, 0.0).astype(jnp.bfloat16)
                    for l in range(lines)
                ],
                axis=1,
            )
            return jnp.dot(
                chosen, halves_v[pl.ds(w * wide, wide), :], preferred_element_type=jnp.float32
            )

        if total == wide:
            acc = pick(0)
        else:
            acc = lax.fori_loop(
                0, total // wide, lambda w, a: a + pick(w), jnp.zeros((ROWS, 2 * LANES), jnp.float32)
            )
        column = acc[:, :LANES] * float(LANES) + acc[:, LANES:]
        for h in range(halves):
            turned = jnp.transpose(column[h * LANES : (h + 1) * LANES, :])
            lane_i[pl.ds(b * halves + h, 1), :] = turned[0:1, :].astype(jnp.int32)
        avg_v[pl.ds(b * ROWS, ROWS), :] = average(lambda w: same_part(column, w))
        store_avg(b).start()

    each(0, blocks, ordered)
    store_lane.start()

    def finish_forward(step):
        for hop in range(1, groups):
            to_group(step * joined, hop).wait_send()

    each(0, turns, finish_forward)
    each(1, members, lambda step: (to_member(step).wait_send(), slots_to(step).wait_send())[0])
    for hop in range(1, groups):
        slots_to_group(hop).wait_send()
    store_lane.wait()
    each(0, blocks, lambda b: store_avg(b).wait())
    local_r.wait()
    each(1, members, lambda step: back_to(step).wait_send())
    each(1, members, lambda step: back_from(step).wait_recv())


def place_kernel(total, avg_ref, slot_ref, back_ref, out_ref, returned_ref, table, rows, slot_s, back_v, in_sem, sems):
    unroll = LANES
    load_s = pltpu.make_async_copy(slot_ref, slot_s, in_sem.at[0])
    load_a = pltpu.make_async_copy(avg_ref, rows, in_sem.at[1])
    load_b = pltpu.make_async_copy(back_ref, back_v, in_sem.at[2])
    store_b = pltpu.make_async_copy(back_v, returned_ref, in_sem.at[3])
    load_s.start()
    load_a.start()
    load_b.start()
    table[...] = jnp.zeros_like(table)
    load_s.wait()
    load_a.wait()

    chunks = total // unroll
    pieces = sems.shape[0]
    size = BUCKET // pieces

    def more(bound, i):
        return jnp.logical_and(i < chunks, slot_s[jnp.minimum(i, chunks - 1), 0] < bound)

    def step(i):
        base = pl.multiple_of(i * unroll, unroll)
        for k in range(unroll):
            s = slot_s[i, k]
            table[pl.ds(s, 1), :] = rows[pl.ds(base + k, 1), :]
        return i + 1

    copies = []
    at = jnp.int32(0)
    for k in range(pieces):
        at = lax.while_loop(functools.partial(more, (k + 1) * size), step, at)
        copy = pltpu.make_async_copy(
            table.at[pl.ds(k * size, size)], out_ref.at[pl.ds(k * size, size)], sems.at[k]
        )
        copy.start()
        copies.append(copy)
        if k == 0:
            load_b.wait()
            store_b.start()
    store_b.wait()
    for copy in copies:
        copy.wait()


def per_device(groups, members, values, slots, counts):
    cap, lanes = values.shape[2:]
    total = groups * members * cap
    hbm = pl.BlockSpec(memory_space=pl.ANY)
    dma = pltpu.SemaphoreType.DMA
    avg, lane_slots, back = pl.pallas_call(
        functools.partial(exchange_kernel, groups, members, cap),
        out_shape=(
            jax.ShapeDtypeStruct((total, lanes), jnp.float32),
            jax.ShapeDtypeStruct((total // LANES, LANES), jnp.int32),
            jax.ShapeDtypeStruct((members, cap, lanes), jnp.bfloat16),
        ),
        in_specs=[hbm, hbm, hbm],
        out_specs=(hbm, hbm, hbm),
        scratch_shapes=[
            pltpu.VMEM((groups * members, cap, lanes), jnp.bfloat16),
            pltpu.VMEM((groups * members, 1, LANES), jnp.int32),
            pltpu.VMEM((members, cap, lanes), jnp.bfloat16),
            pltpu.VMEM((members, 1, LANES), jnp.int32),
            pltpu.VMEM((members, cap), jnp.int32),
            pltpu.SMEM((1, members), jnp.int32),
            pltpu.VMEM((total // LANES, LANES), jnp.int32),
            pltpu.VMEM((total // LANES, LANES), jnp.float32),
            pltpu.VMEM((total // LANES, LANES), jnp.float32),
            pltpu.VMEM((total // LANES, LANES), jnp.float32),
            pltpu.VMEM((total, 2 * LANES), jnp.bfloat16),
            pltpu.VMEM((ROWS, min(WIDE, total)), jnp.bfloat16),
            pltpu.VMEM((total, lanes), jnp.float32),
            pltpu.VMEM((members, cap, lanes), jnp.bfloat16),
            dma((members,)), dma((members,)), dma((members,)), dma((members,)),
            dma((members, groups)), dma((members, groups)), dma((groups,)), dma((groups,)),
            dma((members,)), dma((members,)), dma((3,)), dma((total // ROWS,)),
        ],
        compiler_params=pltpu.CompilerParams(collective_id=0, has_side_effects=True),
    )(values, slots, counts)
    averaged, returned = pl.pallas_call(
        functools.partial(place_kernel, total),
        out_shape=(
            jax.ShapeDtypeStruct((BUCKET, lanes), jnp.float32),
            jax.ShapeDtypeStruct((members, cap, lanes), jnp.bfloat16),
        ),
        in_specs=[hbm, hbm, hbm],
        out_specs=(hbm, hbm),
        scratch_shapes=[
            pltpu.VMEM((BUCKET + 8, lanes), jnp.float32),
            pltpu.VMEM((total, lanes), jnp.float32),
            pltpu.SMEM((total // LANES, LANES), jnp.int32),
            pltpu.VMEM((members, cap, lanes), jnp.bfloat16),
            dma((4,)), dma((8,)),
        ],
    )(avg, lane_slots, back)
    return averaged, returned[None]


def solution(mesh):
    return jax.shard_map(
        functools.partial(per_device, mesh.shape["grp"], mesh.shape["mem"]),
        mesh=mesh,
        in_specs=(
            P(("grp", "mem"), None, None, None),
            P(("grp", "mem"), None, None),
            P(("grp", "mem"), None),
        ),
        out_specs=(P("mem", None), P(("grp", "mem"), None, None, None)),
        check_vma=False,
    )
```
